256 devices in a mesh: rows: 64 (over x, z, core), cols: 4 (over y).
Axes of the slice: x: 4, y: 4, z: 8, core: 2. Of those that a mesh axis runs over, the one named last changes fastest.
Arguments:
- rhs: float32 [2, 32768, 512], P(None, 'rows', 'cols'), may hold values from -6 to 6
- diag_blocks: float32 [2, 512, 512], replicated, may hold values from -0.25 to 0.25
- multipliers: float32 [2, 2, 32768, 512], P(None, None, 'rows'), may hold values from -0.25 to 0.25
- pivots: int32 [1024], P('cols'), may hold values from 0 to 65535, as said below
Outputs:
- solved: float32 [2, 32768, 512], P(None, 'rows', 'cols')
The draws below stay inside these ranges and needn't reach their ends.
Inputs may be any that keep to these rules, and one draw needn't show every extreme that they name: pivots[i] is i or a row at 1024 or beyond; the rows at 1024 or beyond that pivots names are all different, and at most 24 of them lie among the rows held by one index of rows, a number that some index reaches.
All inputs are finite; a program needn't handle non-finite values.
Results may differ from the reference program's by a relative error of at most 0.0001.
Values sent between devices are 32-bit elements; how exact they have to be, the bound alone decides.
No kernel may reach another device: no remote copies, remote signals or barrier semaphores. Data moves between devices by JAX's collectives and lax.ppermute only.
A program may use at most 64 MiB of HBM per device.

```python
import jax
import jax.numpy as jnp
from jax import lax

BLK = 512
PANELS = 2
CYC = 2
R = 512
PB = 1024
MOVE = 24
N_ROWS = 64


def draw_pivots(key, part):
    key_owner, key_slot, key_keep, key_row = jax.random.split(jax.random.fold_in(key, 17), 4)
    places = jnp.arange(PB, dtype=jnp.int32)
    local = CYC * BLK
    chosen = jax.random.randint(key_owner, (), 0, N_ROWS, dtype=jnp.int32)
    slot_count = N_ROWS * MOVE
    slot_ids = jnp.arange(slot_count, dtype=jnp.int32)
    slot_owner = slot_ids // MOVE
    slot_score = jax.random.randint(key_slot, (slot_count,), 0, 32768, dtype=jnp.int32) * slot_count + slot_ids
    slot_score = jnp.where(slot_owner == chosen, 1073741824 + slot_ids, slot_score)
    slot_order = jnp.argsort(slot_score).astype(jnp.int32)
    later = jnp.clip(places - MOVE, 0, slot_count - 1)
    owner = jnp.where(places < MOVE, chosen, slot_owner[slot_order[later]])
    keep = jax.random.randint(key_keep, (PB,), 0, 8, dtype=jnp.int32)
    swapped = (places < MOVE) | (keep != 0)
    owner_ids = jnp.arange(N_ROWS, dtype=jnp.int32)
    hits = ((owner[:, None] == owner_ids[None, :]) & swapped[:, None]).astype(jnp.int32)
    before = jnp.cumsum(hits, axis=0) - hits
    rank = jnp.sum(before * hits, axis=1)
    local_ids = jnp.arange(local, dtype=jnp.int32)
    row_score = jax.random.randint(key_row, (N_ROWS, local), 0, 32768, dtype=jnp.int32) * local + local_ids[None, :]
    barred = (owner_ids[:, None] < PANELS) & (local_ids[None, :] < BLK)
    row_score = jnp.where(barred, 1073741824 + local_ids[None, :], row_score)
    ranked = jnp.argsort(row_score, axis=1).astype(jnp.int32)
    local_row = ranked[owner, jnp.minimum(rank, local - 1)]
    target = local_row // BLK * (N_ROWS * BLK) + owner * BLK + local_row % BLK
    return jnp.where(swapped, target, places).astype(jnp.int32)


def shard_levels(key, dims, shards, smallest, top_value):
    def one(axis_at, parts):
        steps = jax.random.uniform(jax.random.fold_in(jax.random.fold_in(key, 6), axis_at), (parts,), jnp.float32, smallest / len(shards), top_value / len(shards))
        return jnp.repeat(jnp.exp(steps), dims[axis_at] // parts).reshape((-1,) + (1,) * (len(dims) - axis_at - 1))

    gain = one(*shards[0])
    for cut in shards[1:]:
        gain = gain * one(*cut)
    return gain


def normal_values(stream_key, dims, scale, bound, shards=(), held_as=jnp.bfloat16):
    drawn = scale * jax.random.normal(stream_key, dims, jnp.float32)
    if shards:
        drawn = drawn * shard_levels(stream_key, dims, shards, -0.22, 0.18)
    return jnp.clip(drawn, -bound, bound).astype(held_as)


def setup_inputs(seed: int = 0) -> dict:
    arg_keys = jax.random.split(jax.random.key(seed), 5)
    rhs = normal_values(arg_keys[0], (CYC, N_ROWS * BLK, R), 1.0, 6.0, ((1, 64), (2, 4)), jnp.float32)
    diag_blocks = normal_values(arg_keys[1], (PANELS, BLK, BLK), BLK ** -0.5, 0.25, (), jnp.float32)
    multipliers = normal_values(arg_keys[2], (PANELS, CYC, N_ROWS * BLK, BLK), BLK ** -0.5, 0.25, ((2, 64),), jnp.float32)
    pivots = draw_pivots(jax.random.fold_in(arg_keys[4], 71), 0)
    return dict(rhs=rhs, diag_blocks=diag_blocks, multipliers=multipliers, pivots=pivots)


def unit_lower_solve(factor, values):
    return lax.linalg.triangular_solve(factor, values, left_side=True, lower=True, unit_diagonal=True)

def reference(rhs, diag_blocks, multipliers, pivots):
    span = rhs.shape[1]
    width = rhs.shape[2]
    blk = diag_blocks.shape[1]
    total = rhs.shape[0] * span
    whole = rhs.reshape(total, width)

    def interchange(i, order):
        target = pivots[i]
        first = order[i]
        second = order[target]
        return order.at[i].set(second).at[target].set(first)
    order = lax.fori_loop(0, pivots.shape[0], interchange, jnp.arange(total, dtype=jnp.int32))
    permuted = whole[order]
    lower = multipliers.reshape(multipliers.shape[0], total, blk)
    for k in range(multipliers.shape[0]):
        start = k * blk
        finish = start + blk
        panel_rows = unit_lower_solve(diag_blocks[k], permuted[start:finish])
        remain = permuted[finish:] - jnp.dot(lower[k, finish:].astype(jnp.float32), panel_rows.astype(jnp.float32), precision=lax.Precision.HIGHEST, preferred_element_type=jnp.float32)
        permuted = jnp.concatenate([permuted[:start], panel_rows, remain], axis=0)
    return permuted.reshape(rhs.shape)
```

```python
import functools

import jax
import jax.numpy as jnp
from jax import lax
from jax.experimental import pallas as pl
from jax.experimental.pallas import tpu as pltpu
from jax.sharding import PartitionSpec as P

BLK = 512
COLS = 128
MOVE = 24
CHIPS = 32
PLANES = 4
HIGHEST = lax.Precision.HIGHEST
GROUPS = [[2 * chip + core for chip in range(CHIPS)] for core in range(2)]
SWAP = [(device, device ^ 1) for device in range(2 * CHIPS)]
NORTH_TO_SOUTH = [(2 * chip + 1, 2 * chip) for chip in range(CHIPS)]
VMEM = pl.BlockSpec(memory_space=pltpu.VMEM)
SMEM = pl.BlockSpec(memory_space=pltpu.SMEM)
HBM = pl.BlockSpec(memory_space=pl.ANY)


def across_planes(step):
    pairs = []
    for chip in range(CHIPS):
        for plane in range(PLANES):
            device = (2 * chip + 1) * PLANES
            pairs.append((device + plane, device + (plane + step) % PLANES))
    return pairs


def halves(value):
    high = value.astype(jnp.bfloat16)
    return high, (value - high.astype(jnp.float32)).astype(jnp.bfloat16)


def dot(left, right):
    return jnp.dot(left, right, preferred_element_type=jnp.float32)


def product(left_high, left_low, right):
    high, low = halves(right)
    width = right.shape[1]
    both = dot(left_high, jnp.concatenate([high, low], axis=1))
    return both[:, :width] + both[:, width:] + dot(left_low, high)


def stage_kernel(rhs, multipliers, out, sems):
    plane = lax.axis_index("cols")
    copies = [pltpu.make_async_copy(rhs.at[0], out.at[:, 0:16, :], sems.at[0])]
    for part in range(4):
        copies.append(
            pltpu.make_async_copy(
                multipliers.at[0, 0, plane, :, :, pl.ds(128 * part, 128)],
                out.at[pl.ds(8 * part, 8), 16:32, :],
                sems.at[1 + part],
            )
        )
    for copy in copies:
        copy.start()
    for copy in copies:
        copy.wait()


def stage(rhs, multipliers):
    return pl.pallas_call(
        stage_kernel,
        name="stage",
        out_shape=jax.ShapeDtypeStruct((CHIPS, 32, COLS), jnp.float32),
        in_specs=[HBM, HBM],
        out_specs=VMEM,
        scratch_shapes=[pltpu.SemaphoreType.DMA((5,))],
    )(
        rhs.reshape(2, CHIPS, 16, COLS),
        multipliers.reshape(2, 2, PLANES, 8, 16, BLK),
    )


def choose_kernel(pivots, rhs, sent, slots, lists):
    mine = lax.axis_index("rows")
    core = mine % 2
    lane = lax.broadcasted_iota(jnp.int32, (64, 128), 1)
    sub = lax.broadcasted_iota(jnp.int32, (64, 128), 0)
    row = lax.broadcasted_iota(jnp.int32, (128, 128), 0)
    col = lax.broadcasted_iota(jnp.int32, (128, 128), 1)
    earlier = jnp.where(row < col, 1.0, 0.0).astype(jnp.bfloat16)
    carry = jnp.zeros((64, 1), jnp.float32)
    source = jnp.zeros((64, 1), jnp.int32)
    place = jnp.zeros((64, 1), jnp.int32)
    for piece in range(8):
        target = pivots[piece : piece + 1, :]
        owner = lax.shift_right_logical(target, 9) & 63
        moved = target >= 2 * BLK
        hit = (sub == owner) & moved
        ones = jnp.where(hit, 1.0, 0.0)
        before = dot(ones.astype(jnp.bfloat16), earlier) + carry
        carry = carry + jnp.sum(ones, axis=1, keepdims=True)
        rank = jnp.sum(jnp.where(hit, before, 0.0), axis=0, keepdims=True).astype(jnp.int32)
        here = lane[:1] + 128 * piece
        far = jnp.where(owner % 2 == core, 0, CHIPS * MOVE) + (owner // 2) * MOVE + rank
        slots[piece : piece + 1, :] = jnp.where(moved, 2 * BLK + far, here)
        local = lax.shift_right_logical(target, 15) * BLK + (target & (BLK - 1))
        taken = (sub == rank) & moved & (owner == mine)
        source = source + jnp.sum(jnp.where(taken, local + 1, 0), axis=1, keepdims=True)
        place = place + jnp.sum(jnp.where(taken, here + 1, 0), axis=1, keepdims=True)
    source = source[:32] - 1
    place = place[:32] - 1
    lists[...] = jnp.where(lane[:32] == 0, source, place)
    wide = lax.broadcasted_iota(jnp.int32, (32, 2 * BLK), 1)
    pick = jnp.where(wide == source, 1.0, 0.0)
    rows = jnp.dot(pick, rhs[...], precision=HIGHEST, preferred_element_type=jnp.float32)
    sent[...] = jnp.broadcast_to(rows[None, :MOVE], (CHIPS, MOVE, COLS))


def choose(pivots, flat):
    return pl.pallas_call(
        choose_kernel,
        name="choose",
        out_shape=(
            jax.ShapeDtypeStruct((CHIPS, MOVE, COLS), jnp.float32),
            jax.ShapeDtypeStruct((8, 128), jnp.int32),
            jax.ShapeDtypeStruct((32, 128), jnp.int32),
        ),
        in_specs=[VMEM, VMEM],
        out_specs=(VMEM, VMEM, VMEM),
    )(pivots, flat)


def invert_kernel(diag, multipliers, inv_high, inv_low, low_high, low_low, work):
    row = lax.broadcasted_iota(jnp.int32, (128, 128), 0)
    col = lax.broadcasted_iota(jnp.int32, (128, 128), 1)

    def square(left, right):
        return jnp.dot(left, right, precision=HIGHEST, preferred_element_type=jnp.float32)

    def block(panel, i, j):
        return diag[panel, 128 * i : 128 * (i + 1), 128 * j : 128 * (j + 1)]

    for b in range(8):
        pair = (row // 2 == col // 2) & (row > col)
        unit = jnp.where(row == col, 1.0, 0.0)
        work[b] = unit - jnp.where(pair, block(b // 4, b % 4, b % 4), 0.0)

    def level(step, carry):
        shift = step + 1
        near = (lax.shift_right_logical(row, shift) % 2 == 1) & (
            lax.shift_right_logical(col, shift) == lax.shift_right_logical(row, shift) - 1
        )
        firsts = []
        for b in range(8):
            part = jnp.where(near, block(b // 4, b % 4, b % 4), 0.0)
            firsts.append(square(part, work[b]))
        for b in range(8):
            work[b] = work[b] - square(work[b], firsts[b])
        return carry

    lax.fori_loop(0, 6, level, 0)

    def put(panel, i, j, value):
        high, low = halves(value)
        rows = slice(i, i + value.shape[0])
        cols = slice(j, j + value.shape[1])
        inv_high[panel, rows, cols] = high
        inv_low[panel, rows, cols] = low

    zero = jnp.zeros((256, 256), jnp.bfloat16)
    for panel in range(2):
        tops = []
        for half in range(2):
            first = work[4 * panel + 2 * half]
            second = work[4 * panel + 2 * half + 1]
            below = -square(second, square(block(panel, 2 * half + 1, 2 * half), first))
            top = jnp.concatenate([first, jnp.zeros((128, 128), jnp.float32)], axis=1)
            bottom = jnp.concatenate([below, second], axis=1)
            whole = jnp.concatenate([top, bottom], axis=0)
            tops.append(whole)
            put(panel, 256 * half, 256 * half, whole)
        corner = -square(tops[1], square(diag[panel, 256:512, 0:256], tops[0]))
        put(panel, 256, 0, corner)
        inv_high[panel, 0:256, 256:512] = zero
        inv_low[panel, 0:256, 256:512] = zero
    for panel in range(2):
        for cycle in range(2):
            high, low = halves(multipliers[panel, cycle])
            rows = slice(BLK * cycle, BLK * (cycle + 1))
            cols = slice(BLK * panel, BLK * (panel + 1))
            low_high[rows, cols] = high
            low_low[rows, cols] = low


def invert(diag, multipliers):
    return pl.pallas_call(
        invert_kernel,
        name="invert",
        out_shape=(
            jax.ShapeDtypeStruct((2, BLK, BLK), jnp.bfloat16),
            jax.ShapeDtypeStruct((2, BLK, BLK), jnp.bfloat16),
            jax.ShapeDtypeStruct((2 * BLK, 2 * BLK), jnp.bfloat16),
            jax.ShapeDtypeStruct((2 * BLK, 2 * BLK), jnp.bfloat16),
        ),
        in_specs=[VMEM, VMEM],
        out_specs=(VMEM, VMEM, VMEM, VMEM),
        scratch_shapes=[pltpu.VMEM((8, 128, 128), jnp.float32)],
        cost_estimate=pl.CostEstimate(
            flops=4 * 10**9, bytes_accessed=12 * 2**20, transcendentals=0
        ),
    )(diag, multipliers)


def finish_kernel(
    slots, lists, rhs, near, near_other, far, far_other,
    p0, p1, p2, p3, inv_high, inv_low, low_high, low_low,
    out, pool, panel, l21_high, l21_low,
):
    mine = lax.axis_index("rows")
    plane = lax.axis_index("cols")
    core = mine % 2
    own = pl.multiple_of(core * BLK, BLK)
    other = pl.multiple_of(BLK - core * BLK, BLK)
    pool[pl.ds(own, BLK), :] = near[:, :16, :].reshape(BLK, COLS)
    pool[pl.ds(other, BLK), :] = near_other[...].reshape(BLK, COLS)
    pool[2 * BLK : 2 * BLK + CHIPS * MOVE, :] = far[...].reshape(CHIPS * MOVE, COLS)
    pool[2 * BLK + CHIPS * MOVE :, :] = far_other[...].reshape(CHIPS * MOVE, COLS)

    def gather(i, carry):
        for k in range(8):
            spot = i * 8 + k
            panel[pl.ds(spot, 1), :] = pool[pl.ds(slots[spot], 1), :]
        return carry

    lax.fori_loop(0, 2 * BLK // 8, gather, 0)
    for step, pieces in enumerate((p0, p1, p2, p3)):
        base = pl.multiple_of(((plane - step) % PLANES) * 128, 128)
        for part in range(4):
            value = pieces[8 * part : 8 * (part + 1)].reshape(128, 128)
            high, low = halves(value)
            l21_high[pl.ds(base, 128), 128 * part : 128 * (part + 1)] = high
            l21_low[pl.ds(base, 128), 128 * part : 128 * (part + 1)] = low
    first = product(inv_high[0], inv_low[0], panel[:BLK, :])
    rest = panel[BLK:, :] - product(l21_high[...], l21_low[...], first)
    second = product(inv_high[1], inv_low[1], rest)
    solved = jnp.concatenate([first, second], axis=0)
    source = lists[:, 0:1]
    place = lists[:, 1:2]
    wide = lax.broadcasted_iota(jnp.int32, (32, 2 * BLK), 1)
    at_source = jnp.where(wide == source, 1.0, 0.0)
    at_place = jnp.where(wide == place, 1.0, 0.0)
    fresh = jnp.dot(
        at_place, pool[: 2 * BLK, :], precision=HIGHEST, preferred_element_type=jnp.float32
    )
    spread = (((0,), (0,)), ((), ()))
    landed = lax.dot_general(
        at_source, fresh, spread, precision=HIGHEST, preferred_element_type=jnp.float32
    )
    hit = lax.dot_general(
        at_source, jnp.ones((32, COLS), jnp.float32), spread,
        preferred_element_type=jnp.float32,
    )
    base = jnp.where(hit > 0.5, landed, rhs[...])
    result = base - product(low_high[...], low_low[...], solved)
    out[...] = result

    @pl.when(mine == 0)
    def _():
        out[:BLK, :] = first

    @pl.when(mine == 1)
    def _():
        out[:BLK, :] = second


def finish(*operands):
    return pl.pallas_call(
        finish_kernel,
        name="finish",
        out_shape=jax.ShapeDtypeStruct((2 * BLK, COLS), jnp.float32),
        in_specs=[SMEM] + [VMEM] * 14,
        out_specs=VMEM,
        scratch_shapes=[
            pltpu.VMEM((2 * BLK + 2 * CHIPS * MOVE, COLS), jnp.float32),
            pltpu.VMEM((2 * BLK, COLS), jnp.float32),
            pltpu.VMEM((BLK, BLK), jnp.bfloat16),
            pltpu.VMEM((BLK, BLK), jnp.bfloat16),
        ],
    )(*operands)


def exchange(value):
    return lax.all_to_all(value, "rows", 0, 0, axis_index_groups=GROUPS, tiled=True)


def shards(rhs, diag_blocks, multipliers, pivots):
    cycles, blk, columns = rhs.shape
    flat = rhs.reshape(cycles * blk, columns)
    core = lax.axis_index("rows") % 2
    listed = lax.all_to_all(
        jnp.broadcast_to(pivots.reshape(1, 2, 128), (PLANES, 2, 128)),
        "cols", 0, 0, tiled=True,
    ).reshape(8, 128)
    piece = exchange(stage(rhs, multipliers))[0]
    near = exchange(jnp.broadcast_to(piece[None], (CHIPS, 32, COLS)))
    sent, slots, lists = choose(listed, flat)
    far = exchange(sent)
    inverses = invert(diag_blocks, multipliers)
    near_other = lax.ppermute(near[:, :16], "rows", SWAP)
    quarter = near[:, 16:]
    quarters = [quarter] + [
        lax.ppermute(quarter, ("rows", "cols"), across_planes(step)) for step in range(1, 4)
    ]
    down = [lax.ppermute(q, "rows", NORTH_TO_SOUTH) for q in quarters]
    pieces = [jnp.where(core == 1, q, d) for q, d in zip(quarters, down)]
    far_other = lax.ppermute(far, "rows", SWAP)
    solved = finish(
        slots.reshape(1024), lists, flat, near, near_other, far, far_other,
        *pieces, *inverses,
    )
    return solved.reshape(cycles, blk, columns)


def solution(mesh):
    placed = (P(None, "rows", "cols"), P(), P(None, None, "rows", None), P("cols"))
    return jax.shard_map(
        shards, mesh=mesh, in_specs=placed, out_specs=P(None, "rows", "cols"), check_vma=False
    )
```

```python
import jax
import jax.numpy as jnp
from jax import lax
from jax.experimental import pallas as pl
from jax.experimental.pallas import tpu as pltpu
from jax.sharding import PartitionSpec as P

BLK = 512
COLS = 128
MOVE = 24
XS, ZS, PLANES = 4, 8, 4
HEAD = BLK // XS
FAR = ZS * MOVE
FACTOR = 64
HALF = XS * (HEAD + FAR)
HIGHEST = lax.Precision.HIGHEST
VMEM = pl.BlockSpec(memory_space=pltpu.VMEM)
SMEM = pl.BlockSpec(memory_space=pltpu.SMEM)
HBM = pl.BlockSpec(memory_space=pl.ANY)


def device(x, z, core):
    return (x % XS * ZS + z % ZS) * 2 + core


def places():
    return [(x, z, core) for x in range(XS) for z in range(ZS) for core in range(2)]


SWAP = [(device(x, z, c), device(x, z, 1 - c)) for x, z, c in places()]
DOWN = [(device(x, z, 1), device(x, z, 0)) for x, z, c in places() if c == 1]
LINES = [[device(x, z, c) for z in range(ZS)] for x in range(XS) for c in range(2)]


def along_x(step):
    return [(device(x, z, c), device(x + step, z, c)) for x, z, c in places()]


def along_y(step):
    return [(y, (y + step) % PLANES) for y in range(PLANES)]


def from_corner(step):
    return [(device(0, 0, c), device(step, 0, c)) for c in range(2)]


def along_z(*hops):
    return [
        (device(x, start, c), device(x, end, c))
        for start, end in hops
        for x in range(XS)
        for c in range(2)
    ]


def halves(value):
    high = value.astype(jnp.bfloat16)
    return high, (value - high.astype(jnp.float32)).astype(jnp.bfloat16)


def dot(left, right):
    return jnp.dot(left, right, preferred_element_type=jnp.float32)


def product(left_high, left_low, right):
    high, low = halves(right)
    width = right.shape[1]
    both = dot(left_high, jnp.concatenate([high, low], axis=1))
    return both[:, :width] + both[:, width:] + dot(left_low, high)


def times(left, right):
    return product(*halves(left), right)


def stage_kernel(rhs, factor, given, out0, out1, out2, out3, sems):
    core = lax.axis_index("rows") % 2
    plane = lax.axis_index("cols")
    outs = (out0, out1, out2, out3)

    def head(x):
        return pltpu.make_async_copy(
            rhs.at[0, pl.ds(HEAD * x, HEAD), :], outs[x].at[pl.ds(0, HEAD), :], sems.at[5 * x]
        )

    def part(x, col, source, first):
        return pltpu.make_async_copy(
            source.at[pl.ds(first + 16 * x, 16), pl.ds(128 * col, 128)],
            outs[x].at[pl.ds(HEAD + 16 * col, 16), :],
            sems.at[5 * x + 1 + col],
        )

    for x in range(XS):
        head(x).start()

    @pl.when(core == 1)
    def _():
        for x in range(XS):
            for col in range(4):
                part(x, col, factor.at[0, 0], 128 * plane + 64).start()

    @pl.when(core == 0)
    def _():
        for x in range(XS):
            for col in range(4):
                part(x, col, given, 0).start()

    for x in range(XS):
        head(x).wait()
        for col in range(4):
            part(x, col, given, 0).wait()


def stage(rhs, multipliers, given):
    return pl.pallas_call(
        stage_kernel,
        name="stage",
        out_shape=[jax.ShapeDtypeStruct((HEAD + FACTOR, COLS), jnp.float32)] * XS,
        in_specs=[HBM, HBM, HBM],
        out_specs=[VMEM] * XS,
        scratch_shapes=[pltpu.SemaphoreType.DMA((5 * XS,))],
    )(rhs, multipliers, given)


def choose_kernel(piv0, piv1, piv2, piv3, rhs, sent, table):
    mine = lax.axis_index("rows")
    plane = lax.axis_index("cols")
    core = mine % 2
    x_mine = mine // (2 * ZS)
    lane = lax.broadcasted_iota(jnp.int32, (64, 128), 1)
    sub = lax.broadcasted_iota(jnp.int32, (64, 128), 0)
    row = lax.broadcasted_iota(jnp.int32, (128, 128), 0)
    col = lax.broadcasted_iota(jnp.int32, (128, 128), 1)
    earlier = jnp.where(row < col, 1.0, 0.0).astype(jnp.bfloat16)
    carry = jnp.zeros((64, 1), jnp.float32)
    source = jnp.zeros((64, 1), jnp.int32)
    place = jnp.zeros((64, 1), jnp.int32)
    for step, pivots in enumerate((piv0, piv1, piv2, piv3)):
        first = ((plane - step) & 3) * 2
        for half in range(2):
            target = pivots[half : half + 1, :]
            owner = lax.shift_right_logical(target, 9) & 63
            moved = target >= 2 * BLK
            hit = (sub == owner) & moved
            ones = jnp.where(hit, 1.0, 0.0)
            before = dot(ones.astype(jnp.bfloat16), earlier) + carry
            carry = carry + jnp.sum(ones, axis=1, keepdims=True)
            rank = jnp.sum(jnp.where(hit, before, 0.0), axis=0, keepdims=True).astype(jnp.int32)
            here = lane[:1] + 128 * (first + half)
            top = jnp.where(lax.shift_right_logical(here, 9) == core, 0, HALF)
            top = top + ((x_mine - lax.shift_right_logical(here, 7)) & 3) * HEAD + (here & 127)
            far = jnp.where((owner & 1) == core, XS * HEAD, HALF + XS * HEAD)
            far = far + ((x_mine - lax.shift_right_logical(owner, 4)) & 3) * FAR
            far = far + (lax.shift_right_logical(owner, 1) & 7) * MOVE + rank
            table[pl.ds(first + half, 1), :] = jnp.where(moved, far, top)
            local = lax.shift_right_logical(target, 15) * BLK + (target & (BLK - 1))
            taken = (sub == rank) & moved & (owner == mine)
            source = source + jnp.sum(jnp.where(taken, local + 1, 0), axis=1, keepdims=True)
            place = place + jnp.sum(jnp.where(taken, top + 1, 0), axis=1, keepdims=True)
    table[8:9, :] = jnp.sum(jnp.where(lane == sub, source, 0), axis=0, keepdims=True) - 1
    table[9:10, :] = jnp.sum(jnp.where(lane == sub, place, 0), axis=0, keepdims=True) - 1
    wide = lax.broadcasted_iota(jnp.int32, (32, 2 * BLK), 1)
    pick = jnp.where(wide == source[:32] - 1, 1.0, 0.0)
    rows = jnp.dot(pick, rhs[...], precision=HIGHEST, preferred_element_type=jnp.float32)
    sent[...] = jnp.broadcast_to(rows[None, :MOVE], (ZS, MOVE, COLS))


def choose(lists, flat):
    return pl.pallas_call(
        choose_kernel,
        name="choose",
        out_shape=(
            jax.ShapeDtypeStruct((ZS, MOVE, COLS), jnp.float32),
            jax.ShapeDtypeStruct((16, 128), jnp.int32),
        ),
        in_specs=[VMEM] * 5,
        out_specs=(VMEM, VMEM),
    )(*lists, flat)


def small_kernel(diag, out):
    row = lax.broadcasted_iota(jnp.int32, (128, 128), 0)
    col = lax.broadcasted_iota(jnp.int32, (128, 128), 1)

    def block(b):
        first = 128 * (b % 4)
        return diag[b // 4, first : first + 128, first : first + 128]

    for b in range(8):
        pair = (row // 2 == col // 2) & (row > col)
        unit = jnp.where(row == col, 1.0, 0.0)
        out[b] = unit - jnp.where(pair, block(b), 0.0)

    def level(step, carry):
        shift = step + 1
        tile_row = lax.shift_right_logical(row, shift)
        near = (tile_row % 2 == 1) & (lax.shift_right_logical(col, shift) == tile_row - 1)
        firsts = []
        for b in range(8):
            firsts.append(times(jnp.where(near, block(b), 0.0), out[b]))
        for b in range(8):
            out[b] = out[b] - times(out[b], firsts[b])
        return carry

    lax.fori_loop(0, 6, level, 0)


def small_inverses(diag):
    return pl.pallas_call(
        small_kernel,
        name="small_inverses",
        out_shape=jax.ShapeDtypeStruct((8, 128, 128), jnp.float32),
        in_specs=[VMEM],
        out_specs=VMEM,
        cost_estimate=pl.CostEstimate(
            flops=2 * 10**9, bytes_accessed=4 * 2**20, transcendentals=0
        ),
    )(diag)


def grow_kernel(diag, work, multipliers, inv_high, inv_low, low_high, low_low):
    def put(panel, i, j, value):
        high, low = halves(value)
        rows = slice(i, i + value.shape[0])
        cols = slice(j, j + value.shape[1])
        inv_high[panel, rows, cols] = high
        inv_low[panel, rows, cols] = low

    zero = jnp.zeros((256, 256), jnp.bfloat16)
    for panel in range(2):
        tops = []
        for half in range(2):
            first = work[4 * panel + 2 * half]
            second = work[4 * panel + 2 * half + 1]
            at = 256 * half
            below = -times(second, times(diag[panel, at + 128 : at + 256, at : at + 128], first))
            top = jnp.concatenate([first, jnp.zeros((128, 128), jnp.float32)], axis=1)
            bottom = jnp.concatenate([below, second], axis=1)
            whole = jnp.concatenate([top, bottom], axis=0)
            tops.append(whole)
            put(panel, 256 * half, 256 * half, whole)
        corner = -times(tops[1], times(diag[panel, 256:512, 0:256], tops[0]))
        put(panel, 256, 0, corner)
        inv_high[panel, 0:256, 256:512] = zero
        inv_low[panel, 0:256, 256:512] = zero
    for panel in range(2):
        for cycle in range(2):
            high, low = halves(multipliers[panel, cycle])
            rows = slice(BLK * cycle, BLK * (cycle + 1))
            cols = slice(BLK * panel, BLK * (panel + 1))
            low_high[rows, cols] = high
            low_low[rows, cols] = low


def grow(diag, work, multipliers):
    return pl.pallas_call(
        grow_kernel,
        name="grow",
        out_shape=(
            jax.ShapeDtypeStruct((2, BLK, BLK), jnp.bfloat16),
            jax.ShapeDtypeStruct((2, BLK, BLK), jnp.bfloat16),
            jax.ShapeDtypeStruct((2 * BLK, 2 * BLK), jnp.bfloat16),
            jax.ShapeDtypeStruct((2 * BLK, 2 * BLK), jnp.bfloat16),
        ),
        in_specs=[VMEM] * 3,
        out_specs=(VMEM,) * 4,
        cost_estimate=pl.CostEstimate(
            flops=2 * 10**9, bytes_accessed=12 * 2**20, transcendentals=0
        ),
    )(diag, work, multipliers)


def finish_kernel(
    table, rhs, rows_own, rows_other, factor_own, factor_other,
    inv_high, inv_low, low_high, low_low,
    out, pool, panel, l21_high, l21_low,
):
    mine = lax.axis_index("rows")
    plane = lax.axis_index("cols")
    core = mine % 2
    x_mine = mine // (2 * ZS)
    pool[:HALF, :] = rows_own[...]
    pool[HALF:, :] = rows_other[...]
    out[...] = rhs[...]

    def gather(i, carry):
        for k in range(8):
            spot = i * 8 + k
            panel[pl.ds(spot, 1), :] = pool[pl.ds(table[lax.shift_right_logical(spot, 7), spot & 127], 1), :]
        return carry

    lax.fori_loop(0, 2 * BLK // 8, gather, 0)
    for k in range(MOVE):
        source = table[8, k]

        @pl.when(source >= 0)
        def _(source=source, k=k):
            out[pl.ds(source, 1), :] = pool[pl.ds(table[9, k], 1), :]

    for step_y in range(PLANES):
        for step_x in range(XS):
            at = (step_y * XS + step_x) * FACTOR
            for side, source in ((0, factor_own), (1, factor_other)):
                first = ((plane - step_y) & 3) * 128 + ((core + side) & 1) * 64
                first = pl.multiple_of(first + ((x_mine - step_x) & 3) * 16, 16)
                for col in range(4):
                    high, low = halves(source[at + 16 * col : at + 16 * (col + 1), :])
                    l21_high[pl.ds(first, 16), 128 * col : 128 * (col + 1)] = high
                    l21_low[pl.ds(first, 16), 128 * col : 128 * (col + 1)] = low
    first = product(inv_high[0], inv_low[0], panel[:BLK, :])
    rest = panel[BLK:, :] - product(l21_high[...], l21_low[...], first)
    second = product(inv_high[1], inv_low[1], rest)
    solved = jnp.concatenate([first, second], axis=0)
    out[...] = out[...] - product(low_high[...], low_low[...], solved)

    @pl.when(mine == 0)
    def _():
        out[:BLK, :] = first

    @pl.when(mine == 1)
    def _():
        out[:BLK, :] = second


def finish(*operands):
    return pl.pallas_call(
        finish_kernel,
        name="finish",
        out_shape=jax.ShapeDtypeStruct((2 * BLK, COLS), jnp.float32),
        in_specs=[SMEM] + [VMEM] * 9,
        out_specs=VMEM,
        scratch_shapes=[
            pltpu.VMEM((2 * HALF, COLS), jnp.float32),
            pltpu.VMEM((2 * BLK, COLS), jnp.float32),
            pltpu.VMEM((BLK, BLK), jnp.bfloat16),
            pltpu.VMEM((BLK, BLK), jnp.bfloat16),
        ],
    )(*operands)


def spread(value, axis, routes):
    return [value] + [lax.ppermute(value, axis, route) for route in routes]


def shards(rhs, diag_blocks, multipliers, pivots):
    cycles, blk, columns = rhs.shape
    flat = rhs.reshape(cycles * blk, columns)
    mine = lax.axis_index("rows")
    plane = lax.axis_index("cols")
    x_mine = mine // (2 * ZS)
    z_mine = mine // 2 % ZS
    half = lax.dynamic_slice(multipliers[0, 0], (128 * plane, 0), (64, BLK))
    given = lax.ppermute(half, "rows", DOWN)
    lists = spread(pivots.reshape(2, 128), "cols", [along_y(k) for k in (1, 2, 3)])
    staged = stage(rhs, multipliers, given)
    out = [lax.ppermute(staged[k], "rows", from_corner(k)) for k in (1, 2, 3)]
    piece = jnp.where(x_mine == 0, staged[0], out[0] + out[1] + out[2])
    piece = jnp.where(z_mine == 0, piece, 0.0)
    out = [lax.ppermute(piece, "rows", along_z((0, k))) for k in (3, 5)]
    piece = piece + out[0] + out[1]
    out = [
        lax.ppermute(piece, "rows", along_z(*hops))
        for hops in (((0, 1), (3, 2), (5, 6)), ((0, 7), (3, 4)))
    ]
    piece = piece + out[0] + out[1]
    sent, table = choose(lists, flat)
    far = lax.all_to_all(sent, "rows", 0, 0, axis_index_groups=LINES, tiled=True)
    far = far.reshape(FAR, COLS)
    x_routes = [along_x(k) for k in (1, 2, 3)]
    factor = jnp.concatenate(spread(piece[HEAD:], "rows", x_routes))
    tops = spread(jnp.concatenate([piece[:HEAD], far]), "rows", x_routes)
    rows = jnp.concatenate([t[:HEAD] for t in tops] + [t[HEAD:] for t in tops])
    factor = jnp.concatenate(spread(factor, "cols", [along_y(k) for k in (1, 2, 3)]))
    rows_other = lax.ppermute(rows, "rows", SWAP)
    factor_other = lax.ppermute(factor, "rows", SWAP)
    work = small_inverses(diag_blocks)
    inverses = grow(diag_blocks, work, multipliers)
    solved = finish(table, flat, rows, rows_other, factor, factor_other, *inverses)
    return solved.reshape(cycles, blk, columns)


def solution(mesh):
    placed = (P(None, "rows", "cols"), P(), P(None, None, "rows", None), P("cols"))
    return jax.shard_map(
        shards, mesh=mesh, in_specs=placed, out_specs=P(None, "rows", "cols"), check_vma=False
    )
```

```python
import jax
import jax.numpy as jnp
from jax import lax
from jax.experimental import pallas as pl
from jax.experimental.pallas import tpu as pltpu
from jax.sharding import PartitionSpec as P


BLK = 512
COLS = 128
MOVE = 24
XS, ZS, PLANES = 4, 8, 4
HEAD = BLK // XS
FAR = ZS * MOVE
FACTOR = 64
HALF = XS * (HEAD + FAR)
HIGHEST = lax.Precision.HIGHEST
VMEM = pl.BlockSpec(memory_space=pltpu.VMEM)
SMEM = pl.BlockSpec(memory_space=pltpu.SMEM)
HBM = pl.BlockSpec(memory_space=pltpu.HBM)
ROOM = pltpu.CompilerParams(vmem_limit_bytes=24 * 2**20)


def device(x, z, core):
    return (x % XS * ZS + z % ZS) * 2 + core


def places():
    return [(x, z, core) for x in range(XS) for z in range(ZS) for core in range(2)]


SWAP = [(device(x, z, c), device(x, z, 1 - c)) for x, z, c in places()]
DOWN = [(device(x, z, 1), device(x, z, 0)) for x, z, c in places() if c == 1]
LINES = [[device(x, z, c) for z in range(ZS)] for x in range(XS) for c in range(2)]


def along_x(step):
    return [(device(x, z, c), device(x + step, z, c)) for x, z, c in places()]


def along_y(step):
    return [(y, (y + step) % PLANES) for y in range(PLANES)]


def from_corner(step):
    return [(device(0, 0, c), device(step, 0, c)) for c in range(2)]


def along_z(*hops):
    return [
        (device(x, start, c), device(x, end, c))
        for start, end in hops
        for x in range(XS)
        for c in range(2)
    ]


def near(value):
    return pltpu.with_memory_space_constraint(value, pltpu.VMEM)


def away(value):
    return pltpu.with_memory_space_constraint(value, pltpu.HBM)


def halves(value):
    high = value.astype(jnp.bfloat16)
    return high, (value - high.astype(jnp.float32)).astype(jnp.bfloat16)


def dot(left, right):
    return jnp.dot(left, right, preferred_element_type=jnp.float32)


def product(left_high, left_low, right):
    high, low = halves(right)
    width = right.shape[1]
    both = dot(left_high, jnp.concatenate([high, low], axis=1))
    return both[:, :width] + both[:, width:] + dot(left_low, high)


def times(left, right):
    return product(*halves(left), right)


def stage_kernel(rhs, factor, given, out0, out1, out2, out3, sems):
    core = lax.axis_index("rows") % 2
    plane = lax.axis_index("cols")
    outs = (out0, out1, out2, out3)

    def head(x):
        return pltpu.make_async_copy(
            rhs.at[0, pl.ds(HEAD * x, HEAD), :], outs[x].at[pl.ds(0, HEAD), :], sems.at[5 * x]
        )

    def part(x, col, source, first):
        return pltpu.make_async_copy(
            source.at[pl.ds(first + 16 * x, 16), pl.ds(128 * col, 128)],
            outs[x].at[pl.ds(HEAD + 16 * col, 16), :],
            sems.at[5 * x + 1 + col],
        )

    for x in range(XS):
        head(x).start()

    @pl.when(core == 1)
    def _():
        for x in range(XS):
            for col in range(4):
                part(x, col, factor.at[0, 0], 128 * plane + 64).start()

    @pl.when(core == 0)
    def _():
        for x in range(XS):
            for col in range(4):
                part(x, col, given, 0).start()

    for x in range(XS):
        head(x).wait()
        for col in range(4):
            part(x, col, given, 0).wait()


def stage(rhs, multipliers, given):
    return pl.pallas_call(
        stage_kernel,
        name="stage",
        compiler_params=ROOM,
        out_shape=[jax.ShapeDtypeStruct((HEAD + FACTOR, COLS), jnp.float32)] * XS,
        in_specs=[HBM, HBM, VMEM],
        out_specs=[VMEM] * XS,
        scratch_shapes=[pltpu.SemaphoreType.DMA((5 * XS,))],
    )(away(rhs), away(multipliers), near(given))


def choose_kernel(piv0, piv1, piv2, piv3, rhs, sent, table):
    mine = lax.axis_index("rows")
    plane = lax.axis_index("cols")
    core = mine % 2
    x_mine = mine // (2 * ZS)
    lane = lax.broadcasted_iota(jnp.int32, (64, 128), 1)
    sub = lax.broadcasted_iota(jnp.int32, (64, 128), 0)
    row = lax.broadcasted_iota(jnp.int32, (128, 128), 0)
    col = lax.broadcasted_iota(jnp.int32, (128, 128), 1)
    earlier = jnp.where(row < col, 1.0, 0.0).astype(jnp.bfloat16)
    carry = jnp.zeros((64, 1), jnp.float32)
    source = jnp.zeros((64, 1), jnp.int32)
    place = jnp.zeros((64, 1), jnp.int32)
    for step, pivots in enumerate((piv0, piv1, piv2, piv3)):
        first = ((plane - step) & 3) * 2
        for half in range(2):
            target = pivots[half : half + 1, :]
            owner = lax.shift_right_logical(target, 9) & 63
            moved = target >= 2 * BLK
            hit = (sub == owner) & moved
            ones = jnp.where(hit, 1.0, 0.0)
            before = dot(ones.astype(jnp.bfloat16), earlier) + carry
            carry = carry + jnp.sum(ones, axis=1, keepdims=True)
            rank = jnp.sum(jnp.where(hit, before, 0.0), axis=0, keepdims=True).astype(jnp.int32)
            here = lane[:1] + 128 * (first + half)
            top = jnp.where(lax.shift_right_logical(here, 9) == core, 0, HALF)
            top = top + ((x_mine - lax.shift_right_logical(here, 7)) & 3) * HEAD + (here & 127)
            far = jnp.where((owner & 1) == core, XS * HEAD, HALF + XS * HEAD)
            far = far + ((x_mine - lax.shift_right_logical(owner, 4)) & 3) * FAR
            far = far + (lax.shift_right_logical(owner, 1) & 7) * MOVE + rank
            table[pl.ds(first + half, 1), :] = jnp.where(moved, far, top)
            local = lax.shift_right_logical(target, 15) * BLK + (target & (BLK - 1))
            taken = (sub == rank) & moved & (owner == mine)
            source = source + jnp.sum(jnp.where(taken, local + 1, 0), axis=1, keepdims=True)
            place = place + jnp.sum(jnp.where(taken, top + 1, 0), axis=1, keepdims=True)
    table[8:9, :] = jnp.sum(jnp.where(lane == sub, source, 0), axis=0, keepdims=True) - 1
    table[9:10, :] = jnp.sum(jnp.where(lane == sub, place, 0), axis=0, keepdims=True) - 1
    wide = lax.broadcasted_iota(jnp.int32, (32, 2 * BLK), 1)
    pick = jnp.where(wide == source[:32] - 1, 1.0, 0.0)
    rows = jnp.dot(pick, rhs[...], precision=HIGHEST, preferred_element_type=jnp.float32)
    sent[...] = jnp.broadcast_to(rows[None, :MOVE], (ZS, MOVE, COLS))


def choose(lists, flat):
    return pl.pallas_call(
        choose_kernel,
        name="choose",
        compiler_params=ROOM,
        out_shape=(
            jax.ShapeDtypeStruct((ZS, MOVE, COLS), jnp.float32),
            jax.ShapeDtypeStruct((16, 128), jnp.int32),
        ),
        in_specs=[VMEM] * 5,
        out_specs=(VMEM, VMEM),
    )(*map(near, lists), flat)


def invert_kernel(diag, out, work, load):
    core = lax.axis_index("rows") % 2
    copy = pltpu.make_async_copy(diag.at[core], out, load)
    copy.start()
    copy.wait()
    row = lax.broadcasted_iota(jnp.int32, (128, 128), 0)
    col = lax.broadcasted_iota(jnp.int32, (128, 128), 1)

    def block(b):
        return out[128 * b : 128 * (b + 1), 128 * b : 128 * (b + 1)]

    for b in range(4):
        pair = (row // 2 == col // 2) & (row > col)
        unit = jnp.where(row == col, 1.0, 0.0)
        work[b] = unit - jnp.where(pair, block(b), 0.0)

    def level(step, carry):
        shift = step + 1
        tile_row = lax.shift_right_logical(row, shift)
        near = (tile_row % 2 == 1) & (lax.shift_right_logical(col, shift) == tile_row - 1)
        firsts = []
        for b in range(4):
            firsts.append(times(jnp.where(near, block(b), 0.0), work[b]))
        for b in range(4):
            work[b] = work[b] - times(work[b], firsts[b])
        return carry

    lax.fori_loop(0, 6, level, 0)
    tops = []
    for half in range(2):
        first = work[2 * half]
        second = work[2 * half + 1]
        at = 256 * half
        below = -times(second, times(out[at + 128 : at + 256, at : at + 128], first))
        top = jnp.concatenate([first, jnp.zeros((128, 128), jnp.float32)], axis=1)
        bottom = jnp.concatenate([below, second], axis=1)
        tops.append(jnp.concatenate([top, bottom], axis=0))
    out[256:512, 0:256] = -times(tops[1], times(out[256:512, 0:256], tops[0]))
    out[0:256, 0:256] = tops[0]
    out[256:512, 256:512] = tops[1]
    out[0:256, 256:512] = jnp.zeros((256, 256), jnp.float32)


def invert(diag):
    return pl.pallas_call(
        invert_kernel,
        name="invert",
        compiler_params=ROOM,
        out_shape=jax.ShapeDtypeStruct((BLK, BLK), jnp.float32),
        in_specs=[HBM],
        out_specs=VMEM,
        scratch_shapes=[pltpu.VMEM((4, 128, 128), jnp.float32), pltpu.SemaphoreType.DMA],
        cost_estimate=pl.CostEstimate(
            flops=2 * 10**9, bytes_accessed=4 * 2**20, transcendentals=0
        ),
    )(away(diag))


def finish_kernel(
    table, rhs, multipliers, rows_own, rows_other, factor_own, factor_other, inv_own, inv_other,
    out, lower, pool, panel, l21_high, l21_low, inverse, sems,
):
    mine = lax.axis_index("rows")
    plane = lax.axis_index("cols")
    core = mine % 2
    x_mine = mine // (2 * ZS)
    kept = pltpu.make_async_copy(rhs, out, sems.at[0])
    kept.start()
    loads = [pltpu.make_async_copy(multipliers.at[k], lower.at[k], sems.at[1 + k]) for k in range(2)]
    for load in loads:
        load.start()
    pool[:HALF, :] = rows_own[...]
    pool[HALF:, :] = rows_other[...]

    for part in range(8):

        def gather(i, carry, part=part):
            for k in range(8):
                spot = i * 8 + k
                panel[pl.ds(128 * part + spot, 1), :] = pool[pl.ds(table[part, spot], 1), :]
            return carry

        lax.fori_loop(0, 16, gather, 0)
    kept.wait()
    for k in range(MOVE):
        source = table[8, k]

        @pl.when(source >= 0)
        def _(source=source, k=k):
            out[pl.ds(source, 1), :] = pool[pl.ds(table[9, k], 1), :]

    for step_y in range(PLANES):
        for step_x in range(XS):
            at = (step_y * XS + step_x) * FACTOR
            for side, source in ((0, factor_own), (1, factor_other)):
                first = ((plane - step_y) & 3) * 128 + ((core + side) & 1) * 64
                first = pl.multiple_of(first + ((x_mine - step_x) & 3) * 16, 16)
                for col in range(4):
                    high, low = halves(source[at + 16 * col : at + 16 * (col + 1), :])
                    l21_high[pl.ds(first, 16), 128 * col : 128 * (col + 1)] = high
                    l21_low[pl.ds(first, 16), 128 * col : 128 * (col + 1)] = low
    inverse[core] = inv_own[...]
    inverse[1 - core] = inv_other[...]
    first = times(inverse[0], panel[:BLK, :])
    rest = panel[BLK:, :] - product(l21_high[...], l21_low[...], first)
    second = times(inverse[1], rest)
    for load in loads:
        load.wait()
    for cycle in range(2):
        rows = slice(BLK * cycle, BLK * (cycle + 1))
        taken = times(lower[0, cycle], first) + times(lower[1, cycle], second)
        out[rows, :] = out[rows, :] - taken

    @pl.when(mine == 0)
    def _():
        out[:BLK, :] = first

    @pl.when(mine == 1)
    def _():
        out[:BLK, :] = second


def finish(table, flat, multipliers, rows, rows_other, factor, factor_other, inverse, inverse_other):
    return pl.pallas_call(
        finish_kernel,
        name="finish",
        compiler_params=ROOM,
        out_shape=jax.ShapeDtypeStruct((2 * BLK, COLS), jnp.float32),
        in_specs=[SMEM, HBM, HBM] + [VMEM] * 6,
        out_specs=VMEM,
        scratch_shapes=[
            pltpu.VMEM((2, 2, BLK, BLK), jnp.float32),
            pltpu.VMEM((2 * HALF, COLS), jnp.float32),
            pltpu.VMEM((2 * BLK, COLS), jnp.float32),
            pltpu.VMEM((BLK, BLK), jnp.bfloat16),
            pltpu.VMEM((BLK, BLK), jnp.bfloat16),
            pltpu.VMEM((2, BLK, BLK), jnp.float32),
            pltpu.SemaphoreType.DMA((3,)),
        ],
    )(
        table, away(flat), away(multipliers), near(rows), near(rows_other),
        near(factor), near(factor_other), near(inverse), near(inverse_other),
    )


def spread(value, axis, routes):
    return [value] + [lax.ppermute(value, axis, route) for route in routes]


def shards(rhs, diag_blocks, multipliers, pivots):
    cycles, blk, columns = rhs.shape
    flat = rhs.reshape(cycles * blk, columns)
    mine = lax.axis_index("rows")
    plane = lax.axis_index("cols")
    x_mine = mine // (2 * ZS)
    z_mine = mine // 2 % ZS
    half = lax.dynamic_slice(multipliers, (0, 0, 128 * plane, 0), (1, 1, 64, BLK))[0, 0]
    given = lax.ppermute(half, "rows", DOWN)
    lists = spread(pivots.reshape(2, 128), "cols", [along_y(k) for k in (1, 2, 3)])
    staged = stage(rhs, multipliers, given)
    out = [lax.ppermute(staged[k], "rows", from_corner(k)) for k in (1, 2, 3)]
    piece = jnp.where(x_mine == 0, staged[0], out[0] + out[1] + out[2])
    piece = jnp.where(z_mine == 0, piece, 0.0)
    out = [lax.ppermute(piece, "rows", along_z((0, k))) for k in (3, 5)]
    piece = piece + out[0] + out[1]
    out = [
        lax.ppermute(piece, "rows", along_z(*hops))
        for hops in (((0, 1), (3, 2), (5, 6)), ((0, 7), (3, 4)))
    ]
    piece = piece + out[0] + out[1]
    sent, table = choose(lists, flat)
    far = lax.all_to_all(sent, "rows", 0, 0, axis_index_groups=LINES, tiled=True)
    far = far.reshape(FAR, COLS)
    x_routes = [along_x(k) for k in (1, 2, 3)]
    factor = jnp.concatenate(spread(piece[HEAD:], "rows", x_routes))
    tops = spread(jnp.concatenate([piece[:HEAD], far]), "rows", x_routes)
    rows = jnp.concatenate([t[:HEAD] for t in tops] + [t[HEAD:] for t in tops])
    factor = jnp.concatenate(spread(factor, "cols", [along_y(k) for k in (1, 2, 3)]))
    rows_other = lax.ppermute(rows, "rows", SWAP)
    factor_other = lax.ppermute(factor, "rows", SWAP)
    inverse = invert(diag_blocks)
    inverse_other = lax.ppermute(inverse, "rows", SWAP)
    solved = finish(
        table, flat, multipliers, rows, rows_other, factor, factor_other,
        inverse, inverse_other,
    )
    return solved.reshape(cycles, blk, columns)


def solution(mesh):
    placed = (P(None, "rows", "cols"), P(), P(None, None, "rows", None), P("cols"))
    return jax.shard_map(
        shards, mesh=mesh, in_specs=placed, out_specs=P(None, "rows", "cols"), check_vma=False
    )
```

```python
import jax
import jax.numpy as jnp
from jax import lax
from jax.experimental import pallas as pl
from jax.experimental.pallas import tpu as pltpu
from jax.sharding import PartitionSpec as P


BLK = 512
COLS = 128
MOVE = 24
XS, ZS, PLANES = 4, 8, 4
HEAD = BLK // XS
FAR = ZS * MOVE
FACTOR = 64
HALF = XS * (HEAD + FAR)
HIGHEST = lax.Precision.HIGHEST
VMEM = pl.BlockSpec(memory_space=pltpu.VMEM)
SMEM = pl.BlockSpec(memory_space=pltpu.SMEM)
HBM = pl.BlockSpec(memory_space=pltpu.HBM)
ROOM = pltpu.CompilerParams(vmem_limit_bytes=24 * 2**20)


def device(x, z, core):
    return (x % XS * ZS + z % ZS) * 2 + core


def places():
    return [(x, z, core) for x in range(XS) for z in range(ZS) for core in range(2)]


SWAP = [(device(x, z, c), device(x, z, 1 - c)) for x, z, c in places()]
DOWN = [(device(x, z, 1), device(x, z, 0)) for x, z, c in places() if c == 1]


def along_x(step):
    return [(device(x, z, c), device(x + step, z, c)) for x, z, c in places()]


def along_y(step):
    return [(y, (y + step) % PLANES) for y in range(PLANES)]


def from_corner(step):
    return [(device(0, 0, c), device(step, 0, c)) for c in range(2)]


def along_z(*hops):
    return [
        (device(x, start, c), device(x, end, c))
        for start, end in hops
        for x in range(XS)
        for c in range(2)
    ]


def across_z(bit):
    return [(device(x, z, c), device(x, z ^ bit, c)) for x, z, c in places()]


def pick(place, value, *others):
    for spots, other in others:
        here = place == spots[0]
        for spot in spots[1:]:
            here = here | (place == spot)
        value = jnp.where(here, other, value)
    return value


def near(value):
    return pltpu.with_memory_space_constraint(value, pltpu.VMEM)


def away(value):
    return pltpu.with_memory_space_constraint(value, pltpu.HBM)


def halves(value):
    high = value.astype(jnp.bfloat16)
    return high, (value - high.astype(jnp.float32)).astype(jnp.bfloat16)


def dot(left, right):
    return jnp.dot(left, right, preferred_element_type=jnp.float32)


def product(left_high, left_low, right):
    high, low = halves(right)
    width = right.shape[1]
    both = dot(left_high, jnp.concatenate([high, low], axis=1))
    return both[:, :width] + both[:, width:] + dot(left_low, high)


def times(left, right):
    return product(*halves(left), right)


def stage_kernel(rhs, factor, given, out0, out1, out2, out3, sems):
    core = lax.axis_index("rows") % 2
    plane = lax.axis_index("cols")
    outs = (out0, out1, out2, out3)

    def head(x):
        return pltpu.make_async_copy(
            rhs.at[0, pl.ds(HEAD * x, HEAD), :], outs[x].at[pl.ds(0, HEAD), :], sems.at[5 * x]
        )

    def part(x, col, source, first):
        return pltpu.make_async_copy(
            source.at[pl.ds(first + 16 * x, 16), pl.ds(128 * col, 128)],
            outs[x].at[pl.ds(HEAD + 16 * col, 16), :],
            sems.at[5 * x + 1 + col],
        )

    for x in range(XS):
        head(x).start()

    @pl.when(core == 1)
    def _():
        for x in range(XS):
            for col in range(4):
                part(x, col, factor.at[0, 0], 128 * plane + 64).start()

    @pl.when(core == 0)
    def _():
        for x in range(XS):
            for col in range(4):
                part(x, col, given, 0).start()

    for x in range(XS):
        head(x).wait()
        for col in range(4):
            part(x, col, given, 0).wait()


def stage(rhs, multipliers, given):
    return pl.pallas_call(
        stage_kernel,
        name="stage",
        compiler_params=ROOM,
        out_shape=[jax.ShapeDtypeStruct((HEAD + FACTOR, COLS), jnp.float32)] * XS,
        in_specs=[HBM, HBM, VMEM],
        out_specs=[VMEM] * XS,
        scratch_shapes=[pltpu.SemaphoreType.DMA((5 * XS,))],
    )(away(rhs), away(multipliers), near(given))


def choose_kernel(piv0, piv1, piv2, piv3, rhs, sent, table):
    mine = lax.axis_index("rows")
    plane = lax.axis_index("cols")
    core = mine % 2
    x_mine = mine // (2 * ZS)
    z_mine = mine // 2 % ZS
    lane = lax.broadcasted_iota(jnp.int32, (64, 128), 1)
    sub = lax.broadcasted_iota(jnp.int32, (64, 128), 0)
    row = lax.broadcasted_iota(jnp.int32, (128, 128), 0)
    col = lax.broadcasted_iota(jnp.int32, (128, 128), 1)
    earlier = jnp.where(row < col, 1.0, 0.0).astype(jnp.bfloat16)
    carry = jnp.zeros((64, 1), jnp.float32)
    source = jnp.zeros((64, 1), jnp.int32)
    place = jnp.zeros((64, 1), jnp.int32)
    for step, pivots in enumerate((piv0, piv1, piv2, piv3)):
        first = ((plane - step) & 3) * 2
        for half in range(2):
            target = pivots[half : half + 1, :]
            owner = lax.shift_right_logical(target, 9) & 63
            moved = target >= 2 * BLK
            hit = (sub == owner) & moved
            ones = jnp.where(hit, 1.0, 0.0)
            before = dot(ones.astype(jnp.bfloat16), earlier) + carry
            carry = carry + jnp.sum(ones, axis=1, keepdims=True)
            rank = jnp.sum(jnp.where(hit, before, 0.0), axis=0, keepdims=True).astype(jnp.int32)
            here = lane[:1] + 128 * (first + half)
            top = jnp.where(lax.shift_right_logical(here, 9) == core, 0, HALF)
            top = top + ((x_mine - lax.shift_right_logical(here, 7)) & 3) * HEAD + (here & 127)
            far = jnp.where((owner & 1) == core, XS * HEAD, HALF + XS * HEAD)
            far = far + ((x_mine - lax.shift_right_logical(owner, 4)) & 3) * FAR
            far = far + ((lax.shift_right_logical(owner, 1) & 7) ^ z_mine) * MOVE + rank
            table[pl.ds(first + half, 1), :] = jnp.where(moved, far, top)
            local = lax.shift_right_logical(target, 15) * BLK + (target & (BLK - 1))
            taken = (sub == rank) & moved & (owner == mine)
            source = source + jnp.sum(jnp.where(taken, local + 1, 0), axis=1, keepdims=True)
            place = place + jnp.sum(jnp.where(taken, top + 1, 0), axis=1, keepdims=True)
    table[8:9, :] = jnp.sum(jnp.where(lane == sub, source, 0), axis=0, keepdims=True) - 1
    table[9:10, :] = jnp.sum(jnp.where(lane == sub, place, 0), axis=0, keepdims=True) - 1
    wide = lax.broadcasted_iota(jnp.int32, (32, 2 * BLK), 1)
    pick = jnp.where(wide == source[:32] - 1, 1.0, 0.0)
    rows = jnp.dot(pick, rhs[...], precision=HIGHEST, preferred_element_type=jnp.float32)
    sent[...] = rows[:MOVE]


def choose(lists, flat):
    return pl.pallas_call(
        choose_kernel,
        name="choose",
        compiler_params=ROOM,
        out_shape=(
            jax.ShapeDtypeStruct((MOVE, COLS), jnp.float32),
            jax.ShapeDtypeStruct((16, 128), jnp.int32),
        ),
        in_specs=[VMEM] * 5,
        out_specs=(VMEM, VMEM),
    )(*map(near, lists), flat)


def invert_kernel(diag, out, work, load):
    core = lax.axis_index("rows") % 2
    copy = pltpu.make_async_copy(diag.at[core], out, load)
    copy.start()
    copy.wait()
    row = lax.broadcasted_iota(jnp.int32, (128, 128), 0)
    col = lax.broadcasted_iota(jnp.int32, (128, 128), 1)

    def block(b):
        return out[128 * b : 128 * (b + 1), 128 * b : 128 * (b + 1)]

    for b in range(4):
        pair = (row // 2 == col // 2) & (row > col)
        unit = jnp.where(row == col, 1.0, 0.0)
        work[b] = unit - jnp.where(pair, block(b), 0.0)

    def level(step, carry):
        shift = step + 1
        tile_row = lax.shift_right_logical(row, shift)
        near = (tile_row % 2 == 1) & (lax.shift_right_logical(col, shift) == tile_row - 1)
        firsts = []
        for b in range(4):
            firsts.append(times(jnp.where(near, block(b), 0.0), work[b]))
        for b in range(4):
            work[b] = work[b] - times(work[b], firsts[b])
        return carry

    lax.fori_loop(0, 6, level, 0)
    tops = []
    for half in range(2):
        first = work[2 * half]
        second = work[2 * half + 1]
        at = 256 * half
        below = -times(second, times(out[at + 128 : at + 256, at : at + 128], first))
        top = jnp.concatenate([first, jnp.zeros((128, 128), jnp.float32)], axis=1)
        bottom = jnp.concatenate([below, second], axis=1)
        tops.append(jnp.concatenate([top, bottom], axis=0))
    out[256:512, 0:256] = -times(tops[1], times(out[256:512, 0:256], tops[0]))
    out[0:256, 0:256] = tops[0]
    out[256:512, 256:512] = tops[1]
    out[0:256, 256:512] = jnp.zeros((256, 256), jnp.float32)


def invert(diag):
    return pl.pallas_call(
        invert_kernel,
        name="invert",
        compiler_params=ROOM,
        out_shape=jax.ShapeDtypeStruct((BLK, BLK), jnp.float32),
        in_specs=[HBM],
        out_specs=VMEM,
        scratch_shapes=[pltpu.VMEM((4, 128, 128), jnp.float32), pltpu.SemaphoreType.DMA],
        cost_estimate=pl.CostEstimate(
            flops=2 * 10**9, bytes_accessed=4 * 2**20, transcendentals=0
        ),
    )(away(diag))


def finish_kernel(
    table, rhs, multipliers, rows_own, rows_other, factor_own, factor_other, inv_own, inv_other,
    out, lower, pool, panel, l21_high, l21_low, inverse, sems,
):
    mine = lax.axis_index("rows")
    plane = lax.axis_index("cols")
    core = mine % 2
    x_mine = mine // (2 * ZS)
    kept = pltpu.make_async_copy(rhs, out, sems.at[0])
    kept.start()
    loads = [pltpu.make_async_copy(multipliers.at[k], lower.at[k], sems.at[1 + k]) for k in range(2)]
    for load in loads:
        load.start()
    pool[:HALF, :] = rows_own[...]
    pool[HALF:, :] = rows_other[...]

    for part in range(8):

        def gather(i, carry, part=part):
            for k in range(8):
                spot = i * 8 + k
                panel[pl.ds(128 * part + spot, 1), :] = pool[pl.ds(table[part, spot], 1), :]
            return carry

        lax.fori_loop(0, 16, gather, 0)
    kept.wait()
    for k in range(MOVE):
        source = table[8, k]

        @pl.when(source >= 0)
        def _(source=source, k=k):
            out[pl.ds(source, 1), :] = pool[pl.ds(table[9, k], 1), :]

    for step_y in range(PLANES):
        for step_x in range(XS):
            at = (step_y * XS + step_x) * FACTOR
            for side, source in ((0, factor_own), (1, factor_other)):
                first = ((plane - step_y) & 3) * 128 + ((core + side) & 1) * 64
                first = pl.multiple_of(first + ((x_mine - step_x) & 3) * 16, 16)
                for col in range(4):
                    high, low = halves(source[at + 16 * col : at + 16 * (col + 1), :])
                    l21_high[pl.ds(first, 16), 128 * col : 128 * (col + 1)] = high
                    l21_low[pl.ds(first, 16), 128 * col : 128 * (col + 1)] = low
    inverse[core] = inv_own[...]
    inverse[1 - core] = inv_other[...]
    first = times(inverse[0], panel[:BLK, :])
    rest = panel[BLK:, :] - product(l21_high[...], l21_low[...], first)
    second = times(inverse[1], rest)
    for load in loads:
        load.wait()
    for cycle in range(2):
        rows = slice(BLK * cycle, BLK * (cycle + 1))
        taken = times(lower[0, cycle], first) + times(lower[1, cycle], second)
        out[rows, :] = out[rows, :] - taken

    @pl.when(mine == 0)
    def _():
        out[:BLK, :] = first

    @pl.when(mine == 1)
    def _():
        out[:BLK, :] = second


def finish(table, flat, multipliers, rows, rows_other, factor, factor_other, inverse, inverse_other):
    return pl.pallas_call(
        finish_kernel,
        name="finish",
        compiler_params=ROOM,
        out_shape=jax.ShapeDtypeStruct((2 * BLK, COLS), jnp.float32),
        in_specs=[SMEM, HBM, HBM] + [VMEM] * 6,
        out_specs=VMEM,
        scratch_shapes=[
            pltpu.VMEM((2, 2, BLK, BLK), jnp.float32),
            pltpu.VMEM((2 * HALF, COLS), jnp.float32),
            pltpu.VMEM((2 * BLK, COLS), jnp.float32),
            pltpu.VMEM((BLK, BLK), jnp.bfloat16),
            pltpu.VMEM((BLK, BLK), jnp.bfloat16),
            pltpu.VMEM((2, BLK, BLK), jnp.float32),
            pltpu.SemaphoreType.DMA((3,)),
        ],
    )(
        table, away(flat), away(multipliers), near(rows), near(rows_other),
        near(factor), near(factor_other), near(inverse), near(inverse_other),
    )


def spread(value, axis, routes):
    return [value] + [lax.ppermute(value, axis, route) for route in routes]


def shards(rhs, diag_blocks, multipliers, pivots):
    cycles, blk, columns = rhs.shape
    flat = rhs.reshape(cycles * blk, columns)
    mine = lax.axis_index("rows")
    plane = lax.axis_index("cols")
    x_mine = mine // (2 * ZS)
    z_mine = mine // 2 % ZS
    half = lax.dynamic_slice(multipliers, (0, 0, 128 * plane, 0), (1, 1, 64, BLK))[0, 0]
    given = lax.ppermute(half, "rows", DOWN)
    lists = spread(pivots.reshape(2, 128), "cols", [along_y(k) for k in (1, 2, 3)])
    staged = stage(rhs, multipliers, given)
    out = [lax.ppermute(staged[k], "rows", from_corner(k)) for k in (1, 2, 3)]
    piece = pick(x_mine, staged[0], ((1,), out[0]), ((2,), out[1]), ((3,), out[2]))
    out = [lax.ppermute(piece, "rows", along_z((0, k))) for k in (3, 5)]
    piece = pick(z_mine, piece, ((3,), out[0]), ((5,), out[1]))
    out = [
        lax.ppermute(piece, "rows", along_z(*hops))
        for hops in (((0, 1), (3, 2), (5, 6)), ((0, 7), (3, 4)))
    ]
    piece = pick(z_mine, piece, ((1, 2, 6), out[0]), ((7, 4), out[1]))
    far, table = choose(lists, flat)
    for bit in (1, 2, 4):
        far = jnp.concatenate([far, lax.ppermute(far, "rows", across_z(bit))])
    x_routes = [along_x(k) for k in (1, 2, 3)]
    factor = jnp.concatenate(spread(piece[HEAD:], "rows", x_routes))
    tops = spread(jnp.concatenate([piece[:HEAD], far]), "rows", x_routes)
    rows = jnp.concatenate([t[:HEAD] for t in tops] + [t[HEAD:] for t in tops])
    factor = jnp.concatenate(spread(factor, "cols", [along_y(k) for k in (1, 2, 3)]))
    rows_other = lax.ppermute(rows, "rows", SWAP)
    factor_other = lax.ppermute(factor, "rows", SWAP)
    inverse = invert(diag_blocks)
    inverse_other = lax.ppermute(inverse, "rows", SWAP)
    solved = finish(
        table, flat, multipliers, rows, rows_other, factor, factor_other,
        inverse, inverse_other,
    )
    return solved.reshape(cycles, blk, columns)


def solution(mesh):
    placed = (P(None, "rows", "cols"), P(), P(None, None, "rows", None), P("cols"))
    return jax.shard_map(
        shards, mesh=mesh, in_specs=placed, out_specs=P(None, "rows", "cols"), check_vma=False
    )
```

```python
import jax
import jax.numpy as jnp
from jax import lax
from jax.experimental import pallas as pl
from jax.experimental.pallas import tpu as pltpu
from jax.sharding import PartitionSpec as P


BLK = 512
COLS = 128
MOVE = 24
XS, ZS, PLANES = 4, 8, 4
HEAD = BLK // XS
FAR = ZS * MOVE
FACTOR = 64
HALF = XS * (HEAD + FAR)
HIGHEST = lax.Precision.HIGHEST
VMEM = pl.BlockSpec(memory_space=pltpu.VMEM)
SMEM = pl.BlockSpec(memory_space=pltpu.SMEM)
HBM = pl.BlockSpec(memory_space=pltpu.HBM)
ROOM = pltpu.CompilerParams(vmem_limit_bytes=24 * 2**20)


def device(x, z, core):
    return (x % XS * ZS + z % ZS) * 2 + core


def places():
    return [(x, z, core) for x in range(XS) for z in range(ZS) for core in range(2)]


SWAP = [(device(x, z, c), device(x, z, 1 - c)) for x, z, c in places()]
DOWN = [(device(x, z, 1), device(x, z, 0)) for x, z, c in places() if c == 1]


def along_x(step):
    return [(device(x, z, c), device(x + step, z, c)) for x, z, c in places()]


def along_y(step):
    return [(y, (y + step) % PLANES) for y in range(PLANES)]


def from_corner(step):
    return [(device(0, 0, c), device(step, 0, c)) for c in range(2)]


def along_z(*hops):
    return [
        (device(x, start, c), device(x, end, c))
        for start, end in hops
        for x in range(XS)
        for c in range(2)
    ]


def across_z(bit):
    return [(device(x, z, c), device(x, z ^ bit, c)) for x, z, c in places()]


def pick(place, value, *others):
    for spots, other in others:
        here = place == spots[0]
        for spot in spots[1:]:
            here = here | (place == spot)
        value = jnp.where(here, other, value)
    return value


def near(value):
    return pltpu.with_memory_space_constraint(value, pltpu.VMEM)


def away(value):
    return pltpu.with_memory_space_constraint(value, pltpu.HBM)


def halves(value):
    high = value.astype(jnp.bfloat16)
    return high, (value - high.astype(jnp.float32)).astype(jnp.bfloat16)


def dot(left, right):
    return jnp.dot(left, right, preferred_element_type=jnp.float32)


def product(left_high, left_low, right):
    high, low = halves(right)
    width = right.shape[1]
    both = dot(left_high, jnp.concatenate([high, low], axis=1))
    return both[:, :width] + both[:, width:] + dot(left_low, high)


def times(left, right):
    return product(*halves(left), right)


def stage_kernel(rhs, factor, given, out0, out1, out2, out3, sems):
    core = lax.axis_index("rows") % 2
    plane = lax.axis_index("cols")
    outs = (out0, out1, out2, out3)

    def head(x):
        return pltpu.make_async_copy(
            rhs.at[0, pl.ds(HEAD * x, HEAD), :], outs[x].at[pl.ds(0, HEAD), :], sems.at[5 * x]
        )

    def part(x, col, source, first):
        return pltpu.make_async_copy(
            source.at[pl.ds(first + 16 * x, 16), pl.ds(128 * col, 128)],
            outs[x].at[pl.ds(HEAD + 16 * col, 16), :],
            sems.at[5 * x + 1 + col],
        )

    for x in range(XS):
        head(x).start()

    @pl.when(core == 1)
    def _():
        for x in range(XS):
            for col in range(4):
                part(x, col, factor.at[0, 0], 128 * plane + 64).start()

    @pl.when(core == 0)
    def _():
        for x in range(XS):
            for col in range(4):
                part(x, col, given, 0).start()

    for x in range(XS):
        head(x).wait()
        for col in range(4):
            part(x, col, given, 0).wait()


def stage(rhs, multipliers, given):
    return pl.pallas_call(
        stage_kernel,
        name="stage",
        compiler_params=ROOM,
        out_shape=[jax.ShapeDtypeStruct((HEAD + FACTOR, COLS), jnp.float32)] * XS,
        in_specs=[HBM, HBM, VMEM],
        out_specs=[VMEM] * XS,
        scratch_shapes=[pltpu.SemaphoreType.DMA((5 * XS,))],
    )(away(rhs), away(multipliers), near(given))


def choose_kernel(piv0, piv1, piv2, piv3, rhs, sent, table):
    mine = lax.axis_index("rows")
    plane = lax.axis_index("cols")
    core = mine % 2
    x_mine = mine // (2 * ZS)
    z_mine = mine // 2 % ZS
    lane = lax.broadcasted_iota(jnp.int32, (64, 128), 1)
    sub = lax.broadcasted_iota(jnp.int32, (64, 128), 0)
    row = lax.broadcasted_iota(jnp.int32, (128, 128), 0)
    col = lax.broadcasted_iota(jnp.int32, (128, 128), 1)
    earlier = jnp.where(row < col, 1.0, 0.0).astype(jnp.bfloat16)
    carry = jnp.zeros((64, 1), jnp.float32)
    source = jnp.zeros((64, 1), jnp.int32)
    place = jnp.zeros((64, 1), jnp.int32)
    for step, pivots in enumerate((piv0, piv1, piv2, piv3)):
        first = ((plane - step) & 3) * 2
        for half in range(2):
            target = pivots[half : half + 1, :]
            owner = lax.shift_right_logical(target, 9) & 63
            moved = target >= 2 * BLK
            hit = (sub == owner) & moved
            ones = jnp.where(hit, 1.0, 0.0)
            before = dot(ones.astype(jnp.bfloat16), earlier) + carry
            carry = carry + jnp.sum(ones, axis=1, keepdims=True)
            rank = jnp.sum(jnp.where(hit, before, 0.0), axis=0, keepdims=True).astype(jnp.int32)
            here = lane[:1] + 128 * (first + half)
            top = jnp.where(lax.shift_right_logical(here, 9) == core, 0, HALF)
            top = top + ((x_mine - lax.shift_right_logical(here, 7)) & 3) * HEAD + (here & 127)
            far = jnp.where((owner & 1) == core, XS * HEAD, HALF + XS * HEAD)
            far = far + ((x_mine - lax.shift_right_logical(owner, 4)) & 3) * FAR
            far = far + ((lax.shift_right_logical(owner, 1) & 7) ^ z_mine) * MOVE + rank
            table[pl.ds(first + half, 1), :] = jnp.where(moved, far, top)
            local = lax.shift_right_logical(target, 15) * BLK + (target & (BLK - 1))
            taken = (sub == rank) & moved & (owner == mine)
            source = source + jnp.sum(jnp.where(taken, local + 1, 0), axis=1, keepdims=True)
            place = place + jnp.sum(jnp.where(taken, top + 1, 0), axis=1, keepdims=True)
    table[8:9, :] = jnp.sum(jnp.where(lane == sub, source, 0), axis=0, keepdims=True) - 1
    table[9:10, :] = jnp.sum(jnp.where(lane == sub, place, 0), axis=0, keepdims=True) - 1
    wide = lax.broadcasted_iota(jnp.int32, (32, 2 * BLK), 1)
    pick = jnp.where(wide == source[:32] - 1, 1.0, 0.0)
    rows = jnp.dot(pick, rhs[...], precision=HIGHEST, preferred_element_type=jnp.float32)
    sent[...] = rows[:MOVE]


def choose(lists, flat):
    return pl.pallas_call(
        choose_kernel,
        name="choose",
        compiler_params=ROOM,
        out_shape=(
            jax.ShapeDtypeStruct((MOVE, COLS), jnp.float32),
            jax.ShapeDtypeStruct((16, 128), jnp.int32),
        ),
        in_specs=[VMEM] * 5,
        out_specs=(VMEM, VMEM),
    )(*map(near, lists), flat)


def invert_kernel(diag, rhs, multipliers, out, kept, lower, block, work, sems):
    core = lax.axis_index("rows") % 2
    copy = pltpu.make_async_copy(diag.at[core], block, sems.at[0])
    copy.start()
    loads = [
        pltpu.make_async_copy(multipliers, lower, sems.at[1]),
        pltpu.make_async_copy(rhs, kept, sems.at[2]),
    ]
    for load in loads:
        load.start()
    copy.wait()
    row = lax.broadcasted_iota(jnp.int32, (128, 128), 0)
    col = lax.broadcasted_iota(jnp.int32, (128, 128), 1)

    def square(b):
        return block[128 * b : 128 * (b + 1), 128 * b : 128 * (b + 1)]

    for b in range(4):
        pair = (row // 2 == col // 2) & (row > col)
        unit = jnp.where(row == col, 1.0, 0.0)
        work[b] = unit - jnp.where(pair, square(b), 0.0)

    def level(step, carry):
        shift = step + 1
        tile_row = lax.shift_right_logical(row, shift)
        below = (tile_row % 2 == 1) & (lax.shift_right_logical(col, shift) == tile_row - 1)
        firsts = []
        for b in range(4):
            firsts.append(times(jnp.where(below, square(b), 0.0), work[b]))
        for b in range(4):
            work[b] = work[b] - times(work[b], firsts[b])
        return carry

    lax.fori_loop(0, 6, level, 0)
    tops = []
    for half in range(2):
        first = work[2 * half]
        second = work[2 * half + 1]
        at = 256 * half
        below = -times(second, times(block[at + 128 : at + 256, at : at + 128], first))
        top = jnp.concatenate([first, jnp.zeros((128, 128), jnp.float32)], axis=1)
        bottom = jnp.concatenate([below, second], axis=1)
        tops.append(jnp.concatenate([top, bottom], axis=0))
    out[0] = tops[0]
    out[1] = -times(tops[1], times(block[256:512, 0:256], tops[0]))
    out[2] = tops[1]
    for load in loads:
        load.wait()


def invert(diag, flat, multipliers):
    return pl.pallas_call(
        invert_kernel,
        name="invert",
        compiler_params=ROOM,
        out_shape=(
            jax.ShapeDtypeStruct((3, 256, 256), jnp.float32),
            jax.ShapeDtypeStruct((2 * BLK, COLS), jnp.float32),
            jax.ShapeDtypeStruct((2, 2, BLK, BLK), jnp.float32),
        ),
        in_specs=[HBM] * 3,
        out_specs=(VMEM,) * 3,
        scratch_shapes=[
            pltpu.VMEM((BLK, BLK), jnp.float32),
            pltpu.VMEM((4, 128, 128), jnp.float32),
            pltpu.SemaphoreType.DMA((3,)),
        ],
        cost_estimate=pl.CostEstimate(
            flops=2 * 10**9, bytes_accessed=4 * 2**20, transcendentals=0
        ),
    )(away(diag), away(flat), away(multipliers))


def finish_kernel(
    table, kept, lower, rows_own, rows_other, factor_own, factor_other, inv_own, inv_other,
    out, base, pool, panel, l21_high, l21_low, sems,
):
    mine = lax.axis_index("rows")
    plane = lax.axis_index("cols")
    core = mine % 2
    x_mine = mine // (2 * ZS)
    base[...] = kept[...]
    pool[:HALF, :] = rows_own[...]
    pool[HALF:, :] = rows_other[...]
    for part in range(8):
        for spot in range(128):
            panel[pl.ds(128 * part + spot, 1), :] = pool[pl.ds(table[part, spot], 1), :]

    def solve(which, high, low):
        own = core == which
        blocks = [halves(jnp.where(own, inv_own[k], inv_other[k])) for k in range(3)]
        width = high.shape[1]

        def part(block, rows):
            both = dot(block[0], jnp.concatenate([high[rows], low[rows]], axis=1))
            return both[:, :width] + both[:, width:] + dot(block[1], high[rows])

        top, bottom = slice(0, 256), slice(256, 512)
        return jnp.concatenate(
            [part(blocks[0], top), part(blocks[1], top) + part(blocks[2], bottom)], axis=0
        )

    first = solve(0, *halves(panel[:BLK, :]))
    for step_y in range(PLANES):
        for step_x in range(XS):
            at = (step_y * XS + step_x) * FACTOR
            for side, source in ((0, factor_own), (1, factor_other)):
                to = ((plane - step_y) & 3) * 128 + ((core + side) & 1) * 64
                to = pl.multiple_of(to + ((x_mine - step_x) & 3) * 16, 16)
                for col in range(4):
                    high, low = halves(source[at + 16 * col : at + 16 * (col + 1), :])
                    l21_high[pl.ds(to, 16), 128 * col : 128 * (col + 1)] = high
                    l21_low[pl.ds(to, 16), 128 * col : 128 * (col + 1)] = low
    rest = panel[BLK:, :] - product(l21_high[...], l21_low[...], first)
    second = solve(1, *halves(rest))
    for k in range(MOVE):
        source = table[8, k]

        @pl.when(source >= 0)
        def _(source=source, k=k):
            base[pl.ds(source, 1), :] = pool[pl.ds(table[9, k], 1), :]

    stores = []
    for cycle in range(2):
        rows = slice(BLK * cycle, BLK * (cycle + 1))
        taken = times(lower[0, cycle], first) + times(lower[1, cycle], second)
        value = base[rows, :] - taken
        if cycle == 0:
            value = jnp.where(mine == 0, first, jnp.where(mine == 1, second, value))
        base[rows, :] = value
        store = pltpu.make_async_copy(
            base.at[pl.ds(BLK * cycle, BLK)], out.at[pl.ds(BLK * cycle, BLK)], sems.at[cycle]
        )
        store.start()
        stores.append(store)
    for store in stores:
        store.wait()


def finish(table, *operands):
    return pl.pallas_call(
        finish_kernel,
        name="finish",
        compiler_params=ROOM,
        out_shape=jax.ShapeDtypeStruct((2 * BLK, COLS), jnp.float32),
        in_specs=[SMEM] + [VMEM] * 8,
        out_specs=HBM,
        scratch_shapes=[
            pltpu.VMEM((2 * BLK, COLS), jnp.float32),
            pltpu.VMEM((2 * HALF, COLS), jnp.float32),
            pltpu.VMEM((2 * BLK, COLS), jnp.float32),
            pltpu.VMEM((BLK, BLK), jnp.bfloat16),
            pltpu.VMEM((BLK, BLK), jnp.bfloat16),
            pltpu.SemaphoreType.DMA((2,)),
        ],
    )(table, *map(near, operands))


def spread(value, axis, routes):
    return [value] + [lax.ppermute(value, axis, route) for route in routes]


def shards(rhs, diag_blocks, multipliers, pivots):
    cycles, blk, columns = rhs.shape
    flat = rhs.reshape(cycles * blk, columns)
    mine = lax.axis_index("rows")
    plane = lax.axis_index("cols")
    x_mine = mine // (2 * ZS)
    z_mine = mine // 2 % ZS
    half = lax.dynamic_slice(multipliers, (0, 0, 128 * plane, 0), (1, 1, 64, BLK))[0, 0]
    given = lax.ppermute(half, "rows", DOWN)
    lists = spread(pivots.reshape(2, 128), "cols", [along_y(k) for k in (1, 2, 3)])
    staged = stage(rhs, multipliers, given)
    out = [lax.ppermute(staged[k], "rows", from_corner(k)) for k in (1, 2, 3)]
    piece = pick(x_mine, staged[0], ((1,), out[0]), ((2,), out[1]), ((3,), out[2]))
    out = [lax.ppermute(piece, "rows", along_z((0, k))) for k in (3, 5)]
    piece = pick(z_mine, piece, ((3,), out[0]), ((5,), out[1]))
    out = [
        lax.ppermute(piece, "rows", along_z(*hops))
        for hops in (((0, 1), (3, 2), (5, 6)), ((0, 7), (3, 4)))
    ]
    piece = pick(z_mine, piece, ((1, 2, 6), out[0]), ((7, 4), out[1]))
    far, table = choose(lists, flat)
    for bit in (1, 2, 4):
        far = jnp.concatenate([far, lax.ppermute(far, "rows", across_z(bit))])
    x_routes = [along_x(k) for k in (1, 2, 3)]
    factor = jnp.concatenate(spread(piece[HEAD:], "rows", x_routes))
    tops = spread(jnp.concatenate([piece[:HEAD], far]), "rows", x_routes)
    rows = jnp.concatenate([t[:HEAD] for t in tops] + [t[HEAD:] for t in tops])
    factor = jnp.concatenate(spread(factor, "cols", [along_y(k) for k in (1, 2, 3)]))
    rows_other = lax.ppermute(rows, "rows", SWAP)
    factor_other = lax.ppermute(factor, "rows", SWAP)
    inverse, kept, lower = invert(diag_blocks, flat, multipliers)
    inverse_other = lax.ppermute(inverse, "rows", SWAP)
    solved = finish(
        table, kept, lower, rows, rows_other, factor, factor_other,
        inverse, inverse_other,
    )
    return solved.reshape(cycles, blk, columns)


def solution(mesh):
    placed = (P(None, "rows", "cols"), P(), P(None, None, "rows", None), P("cols"))
    return jax.shard_map(
        shards, mesh=mesh, in_specs=placed, out_specs=P(None, "rows", "cols"), check_vma=False
    )
```
